16 devices in a mesh: fsdp: 16 (over z, y, x, core).
Axes of the slice: x: 2, y: 2, z: 2, core: 2. Of those that a mesh axis runs over, the one named last changes fastest.
Arguments:
- tokens: int32 [16, 256], P('fsdp')
- embed_table: float32 [151936, 896], P('fsdp')
- norm_gain: float32 [896], P('fsdp')
- w_query: float32 [896, 896], P('fsdp')
- w_key: float32 [896, 128], P('fsdp')
- w_value: float32 [896, 128], P('fsdp')
- d_query: bfloat16 [16, 256, 896], P('fsdp')
- d_key: bfloat16 [16, 256, 128], P('fsdp')
- d_value: bfloat16 [16, 256, 128], P('fsdp')
Outputs:
- output 1: bfloat16 [16, 256, 896], P('fsdp')
- output 2: bfloat16 [16, 256, 128], P('fsdp')
- output 3: bfloat16 [16, 256, 128], P('fsdp')
- output 4: float32 [151936, 896], P('fsdp')
- output 5: float32 [896], P('fsdp')
- output 6: float32 [896, 896], P('fsdp')
- output 7: float32 [896, 128], P('fsdp')
- output 8: float32 [896, 128], P('fsdp')
All inputs are finite; a program needn't handle non-finite values.
Results may differ from the reference program's by a relative error of at most 0.00452988.
Values are sent between devices in bfloat16 or wider.
A program may use at most 1 GiB of HBM per device.

```python
import math
import jax
import jax.numpy as jnp
from jax import lax

VOCAB_SIZE = 151936
MODEL_DIM = 896
NUM_HEADS = 14
KV_HEADS = 2
HEAD_DIM = 64
BATCH_SIZE = 16
SEQ_LEN = 256


def draw_tokens(tok_key):
    num_levels = int(math.ceil(math.log2(VOCAB_SIZE)))
    level_key, id_key = jax.random.split(tok_key)
    tok_shape = (BATCH_SIZE, SEQ_LEN)
    tok_level = jax.random.randint(level_key, tok_shape, 0, num_levels + 1)
    id_upper = jnp.minimum(jnp.left_shift(jnp.ones(tok_shape, jnp.int32), tok_level), VOCAB_SIZE)
    token_ids = jax.random.randint(id_key, tok_shape, 0, id_upper)
    token_ids = token_ids.at[0, 0].set(0)
    return token_ids.at[BATCH_SIZE - 1, SEQ_LEN - 1].set(VOCAB_SIZE - 1)


def setup_inputs(seed: int = 0) -> dict:
    sub_keys = jax.random.split(jax.random.key(seed), 9)
    q_width = NUM_HEADS * HEAD_DIM
    kv_width = KV_HEADS * HEAD_DIM
    w_scale = MODEL_DIM ** -0.5
    cot_scale = (BATCH_SIZE * SEQ_LEN) ** -0.5
    act_shape = (BATCH_SIZE, SEQ_LEN)
    tokens = draw_tokens(sub_keys[0])
    embed_table = jax.random.normal(sub_keys[1], (VOCAB_SIZE, MODEL_DIM), jnp.float32)
    norm_gain = 1.0 + 0.3 * jax.random.normal(sub_keys[2], (MODEL_DIM,), jnp.float32)
    w_query = w_scale * jax.random.normal(sub_keys[3], (MODEL_DIM, q_width), jnp.float32)
    w_key = w_scale * jax.random.normal(sub_keys[4], (MODEL_DIM, kv_width), jnp.float32)
    w_value = w_scale * jax.random.normal(sub_keys[5], (MODEL_DIM, kv_width), jnp.float32)
    d_query = (cot_scale * jax.random.normal(sub_keys[6], act_shape + (q_width,), jnp.float32)).astype(jnp.bfloat16)
    d_key = (cot_scale * jax.random.normal(sub_keys[7], act_shape + (kv_width,), jnp.float32)).astype(jnp.bfloat16)
    d_value = (cot_scale * jax.random.normal(sub_keys[8], act_shape + (kv_width,), jnp.float32)).astype(jnp.bfloat16)
    return dict(tokens=tokens, embed_table=embed_table, norm_gain=norm_gain, w_query=w_query, w_key=w_key, w_value=w_value, d_query=d_query, d_key=d_key, d_value=d_value)


def reference(tokens, embed_table, norm_gain, w_query, w_key, w_value, d_query, d_key, d_value):
    w_query_bf = w_query.astype(jnp.bfloat16)
    w_key_bf = w_key.astype(jnp.bfloat16)
    w_value_bf = w_value.astype(jnp.bfloat16)

    def seq_step(acc_carry, row_in):
        grad_q, grad_k, grad_v, grad_gain = acc_carry
        tok_row, dq_row, dk_row, dv_row = row_in
        x_rows = embed_table[tok_row].astype(jnp.bfloat16).astype(jnp.float32)
        inv_rms = lax.rsqrt(jnp.mean(x_rows * x_rows, axis=-1, keepdims=True) + 1e-5)
        h_rows = x_rows * inv_rms
        normed = (h_rows * norm_gain).astype(jnp.bfloat16)
        q_rows = jnp.dot(normed, w_query_bf, preferred_element_type=jnp.float32).astype(jnp.bfloat16)
        k_rows = jnp.dot(normed, w_key_bf, preferred_element_type=jnp.float32).astype(jnp.bfloat16)
        v_rows = jnp.dot(normed, w_value_bf, preferred_element_type=jnp.float32).astype(jnp.bfloat16)
        grad_q = grad_q + jnp.dot(normed.T, dq_row, preferred_element_type=jnp.float32)
        grad_k = grad_k + jnp.dot(normed.T, dk_row, preferred_element_type=jnp.float32)
        grad_v = grad_v + jnp.dot(normed.T, dv_row, preferred_element_type=jnp.float32)
        d_normed = (jnp.dot(dq_row, w_query_bf.T, preferred_element_type=jnp.float32)
                    + jnp.dot(dk_row, w_key_bf.T, preferred_element_type=jnp.float32)
                    + jnp.dot(dv_row, w_value_bf.T, preferred_element_type=jnp.float32))
        grad_gain = grad_gain + jnp.sum(d_normed * h_rows, axis=0)
        u_rows = d_normed * norm_gain
        d_x = inv_rms * (u_rows - h_rows * jnp.mean(u_rows * h_rows, axis=-1, keepdims=True))
        return (grad_q, grad_k, grad_v, grad_gain), (q_rows, k_rows, v_rows, d_x)

    acc_init = (jnp.zeros(w_query.shape, jnp.float32), jnp.zeros(w_key.shape, jnp.float32),
                jnp.zeros(w_value.shape, jnp.float32), jnp.zeros(norm_gain.shape, jnp.float32))
    grad_sums, per_row = lax.scan(seq_step, acc_init, (tokens, d_query, d_key, d_value))
    query_proj, key_proj, value_proj, d_x_all = per_row
    d_embed = jnp.zeros(embed_table.shape, jnp.float32).at[tokens].add(d_x_all)
    grad_q, grad_k, grad_v, grad_gain = grad_sums
    return (query_proj, key_proj, value_proj, d_embed, grad_gain, grad_q, grad_k, grad_v)
```

```python
import functools
import jax
import jax.numpy as jnp
from jax import lax
from jax.experimental import pallas as pl
from jax.experimental.pallas import tpu as pltpu
from jax.sharding import PartitionSpec as P

AXIS_NAME = "fsdp"
NDEV = 16
STRIDES = (2, 4, 8)
MESH = pl.DeviceIdType.MESH
SEQ = 256
DM = 896
DF = 1152
WROWS = 56
F32 = jnp.float32
BF16 = jnp.bfloat16


def flip(me, stride):
    return me + stride * (1 - 2 * ((me // stride) % 2))


def flip_mask(me, mask, order=(0, 1, 2)):
    for pos in range(3):
        if (mask >> pos) & 1:
            me = flip(me, STRIDES[order[pos]])
    return me


def colour_order(c):
    return (c, (c + 1) % 3, (c + 2) % 3)


def remote(src, dst, send, recv, dev):
    return pltpu.make_async_remote_copy(src_ref=src, dst_ref=dst, send_sem=send, recv_sem=recv,
                                        device_id=(dev,), device_id_type=MESH)


def barrier_all(me):
    sem = pltpu.get_barrier_semaphore()
    for k in range(1, NDEV):
        pl.semaphore_signal(sem, inc=1, device_id=((me + k) % NDEV,), device_id_type=MESH)
    pl.semaphore_wait(sem, NDEV - 1)


class Gather:
    def __init__(self, me, src, dst, sems, width):
        self.me, self.src, self.dst, self.width = me, src, dst, width
        self.send, self.recv, self.csend, self.crecv = sems

    def cols(self, c):
        return pl.ds(c * self.width, self.width)

    def block(self, c, mask, base=None):
        origin = flip_mask(self.me if base is None else base, mask, colour_order(c))
        return self.dst.at[origin, :, self.cols(c)]

    def link_copy(self, c, mask, pos):
        src = self.src.at[:, self.cols(c)] if mask == 0 else self.block(c, mask)
        new = mask | (1 << pos)
        return remote(src, self.block(c, mask), self.send.at[c, new], self.recv.at[c, new],
                      flip(self.me, STRIDES[colour_order(c)[pos]]))

    def core_copy(self, c, mask):
        src = self.src.at[:, self.cols(c)] if mask == 0 else self.block(c, mask)
        return remote(src, self.block(c, mask), self.csend.at[c, mask], self.crecv.at[c, mask], flip(self.me, 1))

    def start_piece(self, c, mask):
        for pos in range(mask.bit_length(), 3):
            self.link_copy(c, mask, pos).start()
        self.core_copy(c, mask).start()

    def wait_piece(self, c, mask):
        pos = mask.bit_length() - 1
        self.link_copy(c, mask & ~(1 << pos), pos).wait_recv()

    def finish(self):
        for c in range(3):
            for mask in range(8):
                for pos in range(mask.bit_length(), 3):
                    self.link_copy(c, mask, pos).wait_send()
                self.core_copy(c, mask).wait()


def gather_kernel(tok, gain, w, d, tok_o, gain_o, w_o, d_o, small_send, small_recv, loc,
                  ws, wr, wcs, wcr, ds, dr, dcs, dcr):
    me = lax.axis_index(AXIS_NAME)
    own = [pltpu.make_async_copy(tok, tok_o.at[me], loc.at[0]), pltpu.make_async_copy(gain, gain_o.at[me], loc.at[1]),
           pltpu.make_async_copy(w, w_o.at[me], loc.at[2]), pltpu.make_async_copy(d, d_o.at[me], loc.at[3])]
    for copy in own:
        copy.start()
    barrier_all(me)
    small = []
    for k in range(1, NDEV):
        dev = (me + k) % NDEV
        small.append(remote(tok, tok_o.at[me], small_send.at[0, k], small_recv.at[0, k], dev))
        small.append(remote(gain, gain_o.at[me], small_send.at[1, k], small_recv.at[1, k], dev))
    for copy in small:
        copy.start()
    wg = Gather(me, w, w_o, (ws, wr, wcs, wcr), DF // 3)
    dg = Gather(me, d, d_o, (ds, dr, dcs, dcr), DF // 3)
    for g in (wg, dg):
        for c in range(3):
            g.start_piece(c, 0)
    for mask in range(1, 8):
        for g in (wg, dg):
            for c in range(3):
                g.wait_piece(c, mask)
                g.start_piece(c, mask)
    wg.finish()
    dg.finish()
    for copy in small:
        copy.wait()
    for copy in own:
        copy.wait()


def gather_all(tok, gain, w, d):
    vm = pl.BlockSpec(memory_space=pltpu.VMEM)
    hbm = pl.BlockSpec(memory_space=pl.ANY)
    dma = pltpu.SemaphoreType.DMA
    return pl.pallas_call(
        gather_kernel,
        out_shape=(jax.ShapeDtypeStruct((NDEV, 1, SEQ), jnp.int32), jax.ShapeDtypeStruct((NDEV, 1, 128), F32),
                   jax.ShapeDtypeStruct((NDEV, WROWS, DF), BF16), jax.ShapeDtypeStruct((NDEV, SEQ, DF), BF16)),
        in_specs=[vm] * 4,
        out_specs=(hbm,) * 4,
        scratch_shapes=[dma((2, NDEV)), dma((2, NDEV)), dma((4,))] + [dma((3, 8))] * 8,
        compiler_params=pltpu.CompilerParams(collective_id=0, has_side_effects=True),
        name="gather_all",
    )(tok, gain, w, d)


class Scatter:
    def __init__(self, me, part, acc, bufs, sems, piece):
        self.me, self.part, self.acc, self.piece = me, part, acc, piece
        self.r0, self.r = bufs[0], bufs[1:]
        self.csend, self.crecv, self.send, self.recv = sems

    def core_copy(self, mask):
        block = flip_mask(flip(self.me, 1), mask)
        return remote(self.part(block), self.r0.at[mask], self.csend.at[mask], self.crecv.at[mask], flip(self.me, 1))

    def phase_copy(self, c, phase, rel):
        order = colour_order(c)
        absmask = sum(1 << order[pos] for pos in range(3) if (rel >> pos) & 1)
        low = rel >> (phase + 1)
        sem = (0, 4, 6)[phase] + low
        return remote(self.piece(self.acc.at[absmask], c), self.piece(self.r[phase].at[low], c),
                      self.send.at[c, sem], self.recv.at[c, sem], flip(self.me, STRIDES[order[phase]]))

    def core_start(self):
        for mask in (7, 3, 6, 5, 1, 2, 4, 0):
            self.core_copy(mask).start()

    def core_done(self, mask):
        self.core_copy(mask).wait_recv()
        self.acc[mask] = self.part(flip_mask(self.me, mask))[...] + self.r0[mask]
        for c in range(3):
            if (mask >> c) & 1:
                order = colour_order(c)
                rel = sum(1 << pos for pos in range(3) if (mask >> order[pos]) & 1)
                self.phase_copy(c, 0, rel).start()

    def phase_done(self, c, phase, low):
        order = colour_order(c)
        rel = low << (phase + 1)
        self.phase_copy(c, phase, rel | (1 << phase)).wait_recv()
        absmask = sum(1 << order[pos] for pos in range(3) if (rel >> pos) & 1)
        dst = self.piece(self.acc.at[absmask], c)
        dst[...] = dst[...] + self.piece(self.r[phase].at[low], c)[...]

    def move_on(self, c, phase, rel):
        self.phase_copy(c, phase, rel).start()

    def steps(self):
        out = [functools.partial(self.core_done, mask) for mask in (7, 3, 6, 5, 1, 2, 4, 0)]

        def phase0(c, low):
            self.phase_done(c, 0, low)
            if low & 1:
                self.move_on(c, 1, low << 1)

        def phase1(c, low):
            self.phase_done(c, 1, low)
            if low & 1:
                self.move_on(c, 2, low << 2)

        for low in (3, 1, 2, 0):
            out += [functools.partial(phase0, c, low) for c in range(3)]
        for low in (1, 0):
            out += [functools.partial(phase1, c, low) for c in range(3)]
        out += [functools.partial(self.phase_done, c, 2, 0) for c in range(3)]
        return out

    def finish(self):
        for mask in range(8):
            self.core_copy(mask).wait_send()
        for c in range(3):
            for phase in range(3):
                for low in range(4 >> phase):
                    self.phase_copy(c, phase, (low << (phase + 1)) | (1 << phase)).wait_send()


ROW_PIECES = ((0, 96), (96, 80), (176, 80))


def row_piece(ref, c):
    start, size = ROW_PIECES[c]
    return ref.at[pl.ds(start, size)]


def col_piece(ref, c):
    return ref.at[:, pl.ds(c * (DF // 3), DF // 3)]


def step_kernel(xp, g, w, gain, d, qkv_o, dx_o, dw_o, dg_o,
                gbuf, gsem, dxbuf, dxsem, xacc, x0, x1, x2, x3, xcs, xcr, xs, xr,
                dwp, wacc, w0, w1, w2, w3, wcs, wcr, ws, wr, dgp, dgsum, dgall, dgs, dgr):
    me = lax.axis_index(AXIS_NAME)
    load = lambda b, slot: pltpu.make_async_copy(g.at[b], gbuf.at[slot], gsem.at[slot])
    load(0, 0).start()
    dgall[...] = jnp.zeros_like(dgall)
    barrier_all(me)
    xrs = Scatter(me, lambda b: xp.at[b], xacc, (x0, x1, x2, x3), (xcs, xcr, xs, xr), row_piece)
    xrs.core_start()
    events = xrs.steps()
    dgp[...] = jnp.zeros_like(dgp)
    store = lambda b, slot: pltpu.make_async_copy(dxbuf.at[slot], dx_o.at[b], dxsem.at[slot])
    per = -(-len(events) // NDEV)

    @pl.loop(0, NDEV)
    def _(b):
        slot = b % 2

        @pl.when(b + 1 < NDEV)
        def _():
            load(b + 1, 1 - slot).start()

        load(b, slot).wait()

        @pl.when(b >= 2)
        def _():
            store(b - 2, slot).wait()

        dn = lax.dot_general(gbuf[slot], w[...], (((1,), (1,)), ((), ())), preferred_element_type=F32)
        x = xp[b].astype(F32)
        r = lax.rsqrt(jnp.mean(x * x, axis=-1, keepdims=True) + 1e-5)
        h = x * r
        dgp[...] += jnp.sum((dn * h).reshape(SEQ // 8, 8, DM), axis=0)
        u = dn * gain[...]
        dxbuf[slot] = r * (u - h * jnp.mean(u * h, axis=-1, keepdims=True))
        store(b, slot).start()
        for k in range(NDEV):
            group = events[k * per:(k + 1) * per]
            if group:
                @pl.when(b == k)
                def _(group=group):
                    for event in group:
                        event()

    dgsum[...] = jnp.broadcast_to(jnp.sum(dgp[...], axis=0, keepdims=True), dgsum.shape)
    dgall[me] = dgsum[...]
    small = [remote(dgsum.at[pl.ds(0, 1)], dgall.at[me, pl.ds(0, 1)], dgs.at[k], dgr.at[k], (me + k) % NDEV) for k in range(1, NDEV)]
    for copy in small:
        copy.start()
    x = xacc[0].astype(F32)
    r = lax.rsqrt(jnp.mean(x * x, axis=-1, keepdims=True) + 1e-5)
    n = (x * r * gain[...]).astype(BF16)
    dwp[...] = lax.dot_general(n, d[...], (((0,), (0,)), ((), ())), preferred_element_type=F32)
    part = lambda b: dwp.at[pl.ds(pl.multiple_of(b * WROWS, 8), WROWS)]
    wrs = Scatter(me, part, wacc, (w0, w1, w2, w3), (wcs, wcr, ws, wr), col_piece)
    wrs.core_start()
    qkv_o[...] = jnp.dot(n, w[...], preferred_element_type=F32).astype(BF16)
    for event in wrs.steps():
        event()
    dw_o[...] = wacc[0]
    for copy in small:
        copy.wait()
    dg_o[...] = jnp.sum(dgall[...], axis=0)
    store(NDEV - 2, 0).wait()
    store(NDEV - 1, 1).wait()
    xrs.finish()
    wrs.finish()


def step_all(xp, g, w, gain, d):
    vm = pl.BlockSpec(memory_space=pltpu.VMEM)
    hbm = pl.BlockSpec(memory_space=pl.ANY)
    dma = pltpu.SemaphoreType.DMA
    vmem = pltpu.VMEM
    xb = lambda k: vmem((k, SEQ, DM), BF16)
    wb = lambda k: vmem((k, WROWS, DF), F32)
    return pl.pallas_call(
        step_kernel,
        out_shape=(jax.ShapeDtypeStruct((SEQ, DF), BF16), jax.ShapeDtypeStruct((NDEV, SEQ, DM), F32),
                   jax.ShapeDtypeStruct((WROWS, DF), F32), jax.ShapeDtypeStruct((8, DM), F32)),
        in_specs=[vm, hbm, vm, vm, vm],
        out_specs=(vm, hbm, vm, vm),
        scratch_shapes=[vmem((2, SEQ, DF), BF16), dma((2,)), vmem((2, SEQ, DM), F32), dma((2,)),
                        xb(8), xb(8), xb(4), xb(2), xb(1), dma((8,)), dma((8,)), dma((3, 7)), dma((3, 7)),
                        vmem((DM, DF), F32), wb(8), wb(8), wb(4), wb(2), wb(1),
                        dma((8,)), dma((8,)), dma((3, 7)), dma((3, 7)),
                        vmem((8, DM), F32), vmem((8, DM), F32), vmem((NDEV, 8, DM), F32), dma((NDEV,)), dma((NDEV,))],
        compiler_params=pltpu.CompilerParams(collective_id=1, has_side_effects=True, vmem_limit_bytes=62 * 2**20),
        name="step_all",
    )(xp, g, w, gain, d)


def solution(mesh):
    def local_step(tokens, embed_shard, gain_shard, wq_shard, wk_shard, wv_shard, d_query, d_key, d_value):
        vocab_local = embed_shard.shape[0]
        dev_index = lax.axis_index(AXIS_NAME)
        w_shard = jnp.concatenate([wq_shard, wk_shard, wv_shard], axis=1).astype(BF16)
        d_own = jnp.concatenate([d_query[0], d_key[0], d_value[0]], axis=1)
        gain_pad = jnp.pad(gain_shard[None], ((0, 0), (0, 128 - WROWS)))
        tok_all, gain_all, w_all, d_all = gather_all(tokens, gain_pad, w_shard, d_own)
        gain_full = gain_all[:, 0, :WROWS].reshape(1, DM)
        w_full = w_all.reshape(DM, DF)
        local_ids = tok_all[:, 0, :] - dev_index * vocab_local
        is_owned = (local_ids >= 0) & (local_ids < vocab_local)
        owned_rows = jnp.take(embed_shard, jnp.where(is_owned, local_ids, 0), axis=0).astype(BF16)
        part_rows = jnp.where(is_owned[:, :, None], owned_rows, jnp.zeros((), BF16))
        qkv, dx_all, dw, dgain = step_all(part_rows, d_all, w_full, gain_full, d_own)
        scatter_ids = jnp.where(is_owned, local_ids, vocab_local)
        d_embed = jnp.zeros(embed_shard.shape, F32).at[scatter_ids].add(dx_all, mode="drop")
        d_norm_gain = lax.dynamic_slice(dgain, (0, dev_index * WROWS), (1, WROWS))[0]
        return (qkv[None, :, :DM], qkv[None, :, DM:DM + 128], qkv[None, :, DM + 128:], d_embed, d_norm_gain,
                dw[:, :DM], dw[:, DM:DM + 128], dw[:, DM + 128:])

    row_spec = P(AXIS_NAME, None)
    act_spec = P(AXIS_NAME, None, None)
    vec_spec = P(AXIS_NAME)
    return jax.shard_map(local_step, mesh=mesh,
                         in_specs=(row_spec, row_spec, vec_spec, row_spec, row_spec, row_spec, act_spec, act_spec, act_spec),
                         out_specs=(act_spec, act_spec, act_spec, row_spec, vec_spec, row_spec, row_spec, row_spec),
                         check_vma=False)
```

```python
import functools
import jax
import jax.numpy as jnp
from jax import lax
from jax.experimental import pallas as pl
from jax.experimental.pallas import tpu as pltpu
from jax.sharding import PartitionSpec as P

AXIS_NAME = "fsdp"
NDEV = 16
STRIDES = (2, 4, 8)
MESH = pl.DeviceIdType.MESH
SEQ = 256
DM = 896
DF = 1152
WROWS = 56
F32 = jnp.float32
BF16 = jnp.bfloat16


def flip(me, stride):
    return me + stride * (1 - 2 * ((me // stride) % 2))


def flip_mask(me, mask, order=(0, 1, 2)):
    for pos in range(3):
        if (mask >> pos) & 1:
            me = flip(me, STRIDES[order[pos]])
    return me


def colour_order(c):
    return (c, (c + 1) % 3, (c + 2) % 3)


def remote(src, dst, send, recv, dev):
    return pltpu.make_async_remote_copy(src_ref=src, dst_ref=dst, send_sem=send, recv_sem=recv,
                                        device_id=(dev,), device_id_type=MESH)


def barrier_all(me):
    sem = pltpu.get_barrier_semaphore()
    for k in range(1, NDEV):
        pl.semaphore_signal(sem, inc=1, device_id=((me + k) % NDEV,), device_id_type=MESH)
    pl.semaphore_wait(sem, NDEV - 1)


class Gather:
    def __init__(self, me, src, dst, sems, width):
        self.me, self.src, self.dst, self.width = me, src, dst, width
        self.send, self.recv, self.csend, self.crecv = sems

    def cols(self, c):
        return pl.ds(c * self.width, self.width)

    def block(self, c, mask, base=None):
        origin = flip_mask(self.me if base is None else base, mask, colour_order(c))
        return self.dst.at[origin, :, self.cols(c)]

    def link_copy(self, c, mask, pos):
        src = self.src.at[:, self.cols(c)] if mask == 0 else self.block(c, mask)
        new = mask | (1 << pos)
        return remote(src, self.block(c, mask), self.send.at[c, new], self.recv.at[c, new],
                      flip(self.me, STRIDES[colour_order(c)[pos]]))

    def core_copy(self, c, mask):
        src = self.src.at[:, self.cols(c)] if mask == 0 else self.block(c, mask)
        return remote(src, self.block(c, mask), self.csend.at[c, mask], self.crecv.at[c, mask], flip(self.me, 1))

    def start_piece(self, c, mask):
        for pos in range(mask.bit_length(), 3):
            self.link_copy(c, mask, pos).start()
        self.core_copy(c, mask).start()

    def wait_piece(self, c, mask):
        pos = mask.bit_length() - 1
        self.link_copy(c, mask & ~(1 << pos), pos).wait_recv()

    def finish(self):
        for c in range(3):
            for mask in range(8):
                for pos in range(mask.bit_length(), 3):
                    self.link_copy(c, mask, pos).wait_send()
                self.core_copy(c, mask).wait()


def gather_kernel(tok, gain, wq, wk, wv, dq, dk, dv, table, tok_o, gain_o, w_o, d_o, xp_o,
                  wpad, d, ids, tab, rows, xbuf, xsem, small_send, small_recv, loc, ws, wr, wcs, wcr, ds, dr, dcs, dcr):
    me = lax.axis_index(AXIS_NAME)
    vocab = table.shape[0]
    table_copy = pltpu.make_async_copy(table, tab.at[pl.ds(0, vocab)], loc.at[4])
    table_copy.start()
    for ref, src in ((wpad, (wq, wk, wv)), (d, (dq, dk, dv))):
        height = src[0].shape[0]
        ref[:height, :DM] = src[0][...].astype(BF16)
        ref[:height, DM:DM + 128] = src[1][...].astype(BF16)
        ref[:height, DM + 128:] = src[2][...].astype(BF16)
    w = wpad.at[pl.ds(0, WROWS)]
    tab[pl.ds(vocab, 8)] = jnp.zeros((8, DM), F32)
    own = [pltpu.make_async_copy(tok, tok_o.at[me], loc.at[0]), pltpu.make_async_copy(gain, gain_o.at[me], loc.at[1]),
           pltpu.make_async_copy(w, w_o.at[me], loc.at[2]), pltpu.make_async_copy(d, d_o.at[me], loc.at[3])]
    for copy in own:
        copy.start()
    barrier_all(me)
    tok_copies, gain_copies = [], []
    for k in range(1, NDEV):
        dev = (me + k) % NDEV
        tok_copies.append(remote(tok, tok_o.at[me], small_send.at[0, k], small_recv.at[0, k], dev))
        gain_copies.append(remote(gain, gain_o.at[me], small_send.at[1, k], small_recv.at[1, k], dev))
    for copy in tok_copies + gain_copies:
        copy.start()
    wg = Gather(me, w, w_o, (ws, wr, wcs, wcr), DF // 3)
    dg = Gather(me, d, d_o, (ds, dr, dcs, dcr), DF // 3)
    for g in (wg, dg):
        for c in range(3):
            g.start_piece(c, 0)
    for copy in tok_copies:
        copy.wait()
    own[0].wait()
    ids_copy = pltpu.make_async_copy(tok_o, ids, loc.at[5])
    ids_copy.start()

    def piece(g, c, mask):
        g.wait_piece(c, mask)
        g.start_piece(c, mask)

    events = [functools.partial(piece, g, c, mask) for mask in range(1, 8) for g in (wg, dg) for c in range(3)]
    ids_copy.wait()
    table_copy.wait()
    per = -(-len(events) // NDEV)
    store = lambda b, slot: pltpu.make_async_copy(xbuf.at[slot], xp_o.at[b], xsem.at[slot])

    @pl.loop(0, NDEV)
    def _(b):
        slot = b % 2

        @pl.loop(0, SEQ // 8)
        def _(i):
            for j in range(8):
                local = ids[b, 0, i * 8 + j] - me * vocab
                owned = (local >= 0) & (local < vocab)
                rows[pl.ds(i * 8 + j, 1), :] = tab[pl.ds(jnp.where(owned, local, vocab), 1), :]

        @pl.when(b >= 2)
        def _():
            store(b - 2, slot).wait()

        xbuf[slot] = rows[0:SEQ].astype(BF16)
        store(b, slot).start()
        for k in range(NDEV):
            group = events[k * per:(k + 1) * per]
            if group:
                @pl.when(b == k)
                def _(group=group):
                    for event in group:
                        event()

    store(NDEV - 2, 0).wait()
    store(NDEV - 1, 1).wait()
    wg.finish()
    dg.finish()
    for copy in gain_copies + own[1:]:
        copy.wait()


def gather_all(tok, gain, weights, grads, table):
    vm = pl.BlockSpec(memory_space=pltpu.VMEM)
    hbm = pl.BlockSpec(memory_space=pl.ANY)
    dma = pltpu.SemaphoreType.DMA
    vmem = pltpu.VMEM
    return pl.pallas_call(
        gather_kernel,
        out_shape=(jax.ShapeDtypeStruct((NDEV, 1, SEQ), jnp.int32), jax.ShapeDtypeStruct((NDEV, 1, WROWS), F32),
                   jax.ShapeDtypeStruct((NDEV, WROWS, DF), BF16), jax.ShapeDtypeStruct((NDEV, SEQ, DF), BF16),
                   jax.ShapeDtypeStruct((NDEV, SEQ, DM), BF16)),
        in_specs=[vm] * 8 + [hbm],
        out_specs=(hbm,) * 5,
        scratch_shapes=[vmem((64, DF), BF16), vmem((SEQ, DF), BF16), pltpu.SMEM((NDEV, 1, SEQ), jnp.int32),
                        vmem((table.shape[0] + 16, DM), F32), vmem((SEQ + 8, DM), F32), vmem((2, SEQ, DM), BF16), dma((2,)),
                        dma((2, NDEV)), dma((2, NDEV)), dma((6,))] + [dma((3, 8))] * 8,
        compiler_params=pltpu.CompilerParams(collective_id=0, has_side_effects=True, vmem_limit_bytes=56 * 2**20),
        name="gather_all",
    )(tok, gain, *weights, *grads, table)


class Scatter:
    def __init__(self, me, part, acc, bufs, sems, piece):
        self.me, self.part, self.acc, self.piece = me, part, acc, piece
        self.r0, self.r = bufs[0], bufs[1:]
        self.csend, self.crecv, self.send, self.recv = sems

    def core_copy(self, mask):
        block = flip_mask(flip(self.me, 1), mask)
        return remote(self.part(block), self.r0.at[mask], self.csend.at[mask], self.crecv.at[mask], flip(self.me, 1))

    def phase_copy(self, c, phase, rel):
        order = colour_order(c)
        absmask = sum(1 << order[pos] for pos in range(3) if (rel >> pos) & 1)
        low = rel >> (phase + 1)
        sem = (0, 4, 6)[phase] + low
        return remote(self.piece(self.acc.at[absmask], c), self.piece(self.r[phase].at[low], c),
                      self.send.at[c, sem], self.recv.at[c, sem], flip(self.me, STRIDES[order[phase]]))

    def core_start(self):
        for mask in (7, 3, 6, 5, 1, 2, 4, 0):
            self.core_copy(mask).start()

    def core_done(self, mask):
        self.core_copy(mask).wait_recv()
        self.acc[mask] = self.part(flip_mask(self.me, mask))[...] + self.r0[mask]
        for c in range(3):
            if (mask >> c) & 1:
                order = colour_order(c)
                rel = sum(1 << pos for pos in range(3) if (mask >> order[pos]) & 1)
                self.phase_copy(c, 0, rel).start()

    def phase_done(self, c, phase, low):
        order = colour_order(c)
        rel = low << (phase + 1)
        self.phase_copy(c, phase, rel | (1 << phase)).wait_recv()
        absmask = sum(1 << order[pos] for pos in range(3) if (rel >> pos) & 1)
        dst = self.piece(self.acc.at[absmask], c)
        dst[...] = dst[...] + self.piece(self.r[phase].at[low], c)[...]

    def move_on(self, c, phase, rel):
        self.phase_copy(c, phase, rel).start()

    def steps(self):
        out = [functools.partial(self.core_done, mask) for mask in (7, 3, 6, 5, 1, 2, 4, 0)]

        def phase0(c, low):
            self.phase_done(c, 0, low)
            if low & 1:
                self.move_on(c, 1, low << 1)

        def phase1(c, low):
            self.phase_done(c, 1, low)
            if low & 1:
                self.move_on(c, 2, low << 2)

        for low in (3, 1, 2, 0):
            out += [functools.partial(phase0, c, low) for c in range(3)]
        for low in (1, 0):
            out += [functools.partial(phase1, c, low) for c in range(3)]
        out += [functools.partial(self.phase_done, c, 2, 0) for c in range(3)]
        return out

    def finish(self):
        for mask in range(8):
            self.core_copy(mask).wait_send()
        for c in range(3):
            for phase in range(3):
                for low in range(4 >> phase):
                    self.phase_copy(c, phase, (low << (phase + 1)) | (1 << phase)).wait_send()


ROW_PIECES = ((0, 96), (96, 80), (176, 80))


def row_piece(ref, c):
    start, size = ROW_PIECES[c]
    return ref.at[pl.ds(start, size)]


def col_piece(ref, c):
    return ref.at[:, pl.ds(c * (DF // 3), DF // 3)]


def step_kernel(xp, g, w, gain, qkv_o, dx_o, dw_o, dg_o,
                d, dsem, gbuf, gsem, dxbuf, dxsem, xacc, x0, x1, x2, x3, xcs, xcr, xs, xr,
                dwp, wacc, w0, w1, w2, w3, wcs, wcr, ws, wr, dgp, dgsum, dgall, dgs, dgr):
    me = lax.axis_index(AXIS_NAME)
    load = lambda b, slot: pltpu.make_async_copy(g.at[b], gbuf.at[slot], gsem.at[slot])
    load(0, 0).start()
    d_copy = pltpu.make_async_copy(g.at[me], d, dsem)
    d_copy.start()
    dgall[...] = jnp.zeros_like(dgall)
    barrier_all(me)
    xrs = Scatter(me, lambda b: xp.at[b], xacc, (x0, x1, x2, x3), (xcs, xcr, xs, xr), row_piece)
    xrs.core_start()
    events = xrs.steps()
    dgp[...] = jnp.zeros_like(dgp)
    store = lambda b, slot: pltpu.make_async_copy(dxbuf.at[slot], dx_o.at[b], dxsem.at[slot])
    per = -(-len(events) // NDEV)

    @pl.loop(0, NDEV)
    def _(b):
        slot = b % 2

        @pl.when(b + 1 < NDEV)
        def _():
            load(b + 1, 1 - slot).start()

        load(b, slot).wait()

        @pl.when(b >= 2)
        def _():
            store(b - 2, slot).wait()

        dn = lax.dot_general(gbuf[slot], w[...], (((1,), (1,)), ((), ())), preferred_element_type=F32)
        x = xp[b].astype(F32)
        r = lax.rsqrt(jnp.mean(x * x, axis=-1, keepdims=True) + 1e-5)
        h = x * r
        dgp[...] += jnp.sum((dn * h).reshape(SEQ // 8, 8, DM), axis=0)
        u = dn * gain[...]
        dxbuf[slot] = r * (u - h * jnp.mean(u * h, axis=-1, keepdims=True))
        store(b, slot).start()
        for k in range(NDEV):
            group = events[k * per:(k + 1) * per]
            if group:
                @pl.when(b == k)
                def _(group=group):
                    for event in group:
                        event()

    dgsum[...] = jnp.broadcast_to(jnp.sum(dgp[...], axis=0, keepdims=True), dgsum.shape)
    dgall[me] = dgsum[...]
    small = [remote(dgsum.at[pl.ds(0, 1)], dgall.at[me, pl.ds(0, 1)], dgs.at[k], dgr.at[k], (me + k) % NDEV) for k in range(1, NDEV)]
    for copy in small:
        copy.start()
    d_copy.wait()
    x = xacc[0].astype(F32)
    r = lax.rsqrt(jnp.mean(x * x, axis=-1, keepdims=True) + 1e-5)
    n = (x * r * gain[...]).astype(BF16)
    dwp[...] = lax.dot_general(n, d[...], (((0,), (0,)), ((), ())), preferred_element_type=F32)
    part = lambda b: dwp.at[pl.ds(pl.multiple_of(b * WROWS, 8), WROWS)]
    wrs = Scatter(me, part, wacc, (w0, w1, w2, w3), (wcs, wcr, ws, wr), col_piece)
    wrs.core_start()
    qkv_o[...] = jnp.dot(n, w[...], preferred_element_type=F32).astype(BF16)
    for event in wrs.steps():
        event()
    dw_o[...] = wacc[0]
    for copy in small:
        copy.wait()
    dg_o[...] = jnp.sum(dgall[...], axis=0)
    store(NDEV - 2, 0).wait()
    store(NDEV - 1, 1).wait()
    xrs.finish()
    wrs.finish()


def step_all(xp, g, w, gain):
    vm = pl.BlockSpec(memory_space=pltpu.VMEM)
    hbm = pl.BlockSpec(memory_space=pl.ANY)
    dma = pltpu.SemaphoreType.DMA
    vmem = pltpu.VMEM
    xb = lambda k: vmem((k, SEQ, DM), BF16)
    wb = lambda k: vmem((k, WROWS, DF), F32)
    return pl.pallas_call(
        step_kernel,
        out_shape=(jax.ShapeDtypeStruct((SEQ, DF), BF16), jax.ShapeDtypeStruct((NDEV, SEQ, DM), F32),
                   jax.ShapeDtypeStruct((WROWS, DF), F32), jax.ShapeDtypeStruct((8, DM), F32)),
        in_specs=[vm, hbm, vm, vm],
        out_specs=(vm, hbm, vm, vm),
        scratch_shapes=[vmem((SEQ, DF), BF16), dma, vmem((2, SEQ, DF), BF16), dma((2,)), vmem((2, SEQ, DM), F32), dma((2,)),
                        xb(8), xb(8), xb(4), xb(2), xb(1), dma((8,)), dma((8,)), dma((3, 7)), dma((3, 7)),
                        vmem((DM, DF), F32), wb(8), wb(8), wb(4), wb(2), wb(1),
                        dma((8,)), dma((8,)), dma((3, 7)), dma((3, 7)),
                        vmem((8, DM), F32), vmem((8, DM), F32), vmem((NDEV, 8, DM), F32), dma((NDEV,)), dma((NDEV,))],
        compiler_params=pltpu.CompilerParams(collective_id=1, has_side_effects=True, vmem_limit_bytes=62 * 2**20),
        name="step_all",
    )(xp, g, w, gain)


def embed_kernel(keys, starts, dx, qkv, dw, de_o, q_o, k_o, v_o, dwq_o, dwk_o, dwv_o, dxv, de, insem, outsem):
    vocab = de_o.shape[0]
    fetch = pltpu.make_async_copy(dx, dxv.at[pl.ds(0, NDEV * SEQ)], insem)
    fetch.start()

    @pl.loop(0, (vocab + 8) // 32)
    def _(i):
        de[pl.ds(pl.multiple_of(i * 32, 32), 32)] = jnp.zeros((32, DM), F32)

    for outs, ref in (((q_o, k_o, v_o), qkv), ((dwq_o, dwk_o, dwv_o), dw)):
        outs[0][...] = ref[:, :DM]
        outs[1][...] = ref[:, DM:DM + 128]
        outs[2][...] = ref[:, DM + 128:]
    fetch.wait()

    def token(pos, carry):
        prev, total = carry
        key = keys[pos]
        row = lax.shift_right_logical(key, 12)
        part = dxv[pl.ds(key & 4095, 1), :]
        total = jnp.where(row == prev, total, 0.0) + part
        de[pl.ds(row, 1), :] = total
        return row, total

    def group(g, carry):
        first = (starts[0] - 1 - g) * 8
        for j in range(7, -1, -1):
            carry = token(first + j, carry)
        return carry

    carry = (jnp.int32(-1), jnp.zeros((1, DM), F32))
    done = jnp.int32(0)
    copies = []
    bounds = embed_bounds(vocab)
    for k in range(len(bounds) - 1):
        upto = starts[0] - starts[k + 1]
        carry = lax.fori_loop(done, upto, group, carry)
        done = upto
        low, high = bounds[k + 1], bounds[k]
        copies.append(pltpu.make_async_copy(de.at[pl.ds(low, high - low)], de_o.at[pl.ds(low, high - low)], outsem.at[k]))
        copies[-1].start()
    for copy in copies:
        copy.wait()


def embed_bounds(vocab):
    blocks = 16
    return [vocab] + [(vocab * k // blocks) // 8 * 8 for k in range(blocks - 1, 0, -1)] + [0]


def embed_all(local_ids, is_owned, dx, qkv, dw, vocab):
    order = jnp.arange(NDEV * SEQ, dtype=jnp.int32)
    keys = jnp.sort(jnp.where(is_owned, local_ids, vocab).reshape(-1) * 4096 + order)
    bounds = jnp.array(embed_bounds(vocab), jnp.int32)
    below = jnp.sum((keys[None, :] < bounds[:, None] * 4096).astype(jnp.int32), axis=1)
    starts = jnp.concatenate([(below[:1] + 7) // 8, below[1:] // 8])
    vm = pl.BlockSpec(memory_space=pltpu.VMEM)
    hbm = pl.BlockSpec(memory_space=pl.ANY)
    smem = pl.BlockSpec(memory_space=pltpu.SMEM)
    sds = jax.ShapeDtypeStruct
    return pl.pallas_call(
        embed_kernel,
        out_shape=(sds((vocab, DM), F32), sds((SEQ, DM), BF16), sds((SEQ, 128), BF16), sds((SEQ, 128), BF16),
                   sds((WROWS, DM), F32), sds((WROWS, 128), F32), sds((WROWS, 128), F32)),
        in_specs=[smem, smem, hbm, vm, vm],
        out_specs=(hbm,) + (vm,) * 6,
        scratch_shapes=[pltpu.VMEM((NDEV * SEQ + 8, DM), F32), pltpu.VMEM((vocab + 8, DM), F32),
                        pltpu.SemaphoreType.DMA, pltpu.SemaphoreType.DMA((16,))],
        compiler_params=pltpu.CompilerParams(vmem_limit_bytes=60 * 2**20),
        name="embed_all",
    )(keys, starts, dx.reshape(NDEV * SEQ, DM), qkv, dw)


def solution(mesh):
    def local_step(tokens, embed_shard, gain_shard, wq_shard, wk_shard, wv_shard, d_query, d_key, d_value):
        vocab_local = embed_shard.shape[0]
        dev_index = lax.axis_index(AXIS_NAME)
        tok_all, gain_all, w_all, d_all, part_rows = gather_all(
            tokens, gain_shard[None], (wq_shard, wk_shard, wv_shard), (d_query[0], d_key[0], d_value[0]), embed_shard)
        gain_full = gain_all.reshape(1, DM)
        local_ids = tok_all[:, 0, :] - dev_index * vocab_local
        is_owned = (local_ids >= 0) & (local_ids < vocab_local)
        qkv, dx_all, dw, dgain = step_all(part_rows, d_all, w_all.reshape(DM, DF), gain_full)
        d_embed, *small = embed_all(local_ids, is_owned, dx_all, qkv, dw, vocab_local)
        d_norm_gain = lax.dynamic_slice(dgain, (0, dev_index * WROWS), (1, WROWS))[0]
        return (*(a[None] for a in small[:3]), d_embed, d_norm_gain, *small[3:])

    row_spec = P(AXIS_NAME, None)
    act_spec = P(AXIS_NAME, None, None)
    vec_spec = P(AXIS_NAME)
    return jax.shard_map(local_step, mesh=mesh,
                         in_specs=(row_spec, row_spec, vec_spec, row_spec, row_spec, row_spec, act_spec, act_spec, act_spec),
                         out_specs=(act_spec, act_spec, act_spec, row_spec, vec_spec, row_spec, row_spec, row_spec),
                         check_vma=False)
```

```python
import functools
import jax
import jax.numpy as jnp
from jax import lax
from jax.experimental import pallas as pl
from jax.experimental.pallas import tpu as pltpu
from jax.sharding import PartitionSpec as P

AXIS_NAME = "fsdp"
NDEV = 16
STRIDES = (2, 4, 8)
MESH = pl.DeviceIdType.MESH
SEQ = 256
DM = 896
DF = 1152
WROWS = 56
PAIR = 2
STEP = PAIR * SEQ
CHUNK = 64
QUARTERS = 4
SPLIT = 18
F32 = jnp.float32
BF16 = jnp.bfloat16


def flip(me, stride):
    return me + stride * (1 - 2 * ((me // stride) % 2))


def flip_mask(me, mask, order=(0, 1, 2)):
    for pos in range(3):
        if (mask >> pos) & 1:
            me = flip(me, STRIDES[order[pos]])
    return me


def colour_order(c):
    return (c, (c + 1) % 3, (c + 2) % 3)


def remote(src, dst, send, recv, dev):
    return pltpu.make_async_remote_copy(src_ref=src, dst_ref=dst, send_sem=send, recv_sem=recv,
                                        device_id=(dev,), device_id_type=MESH)


def barrier_all(me):
    sem = pltpu.get_barrier_semaphore()
    for k in range(1, NDEV):
        pl.semaphore_signal(sem, inc=1, device_id=((me + k) % NDEV,), device_id_type=MESH)
    pl.semaphore_wait(sem, NDEV - 1)


class Gather:
    def __init__(self, me, src, dst, sems, width):
        self.me, self.src, self.dst, self.width = me, src, dst, width
        self.send, self.recv, self.csend, self.crecv = sems

    def cols(self, c):
        return pl.ds(c * self.width, self.width)

    def block(self, c, mask, base=None):
        origin = flip_mask(self.me if base is None else base, mask, colour_order(c))
        return self.dst.at[origin, :, self.cols(c)]

    def link_copy(self, c, mask, pos):
        src = self.src.at[:, self.cols(c)] if mask == 0 else self.block(c, mask)
        new = mask | (1 << pos)
        return remote(src, self.block(c, mask), self.send.at[c, new], self.recv.at[c, new],
                      flip(self.me, STRIDES[colour_order(c)[pos]]))

    def core_copy(self, c, mask):
        src = self.src.at[:, self.cols(c)] if mask == 0 else self.block(c, mask)
        return remote(src, self.block(c, mask), self.csend.at[c, mask], self.crecv.at[c, mask], flip(self.me, 1))

    def start_piece(self, c, mask):
        for pos in range(mask.bit_length(), 3):
            self.link_copy(c, mask, pos).start()
        self.core_copy(c, mask).start()

    def wait_piece(self, c, mask):
        pos = mask.bit_length() - 1
        self.link_copy(c, mask & ~(1 << pos), pos).wait_recv()

    def finish(self):
        for c in range(3):
            for mask in range(8):
                for pos in range(mask.bit_length(), 3):
                    self.link_copy(c, mask, pos).wait_send()
                self.core_copy(c, mask).wait()


def rotate(x, amount, axis):
    extent = x.shape[axis]
    return jnp.concatenate([lax.slice_in_dim(x, extent - amount, extent, axis=axis),
                            lax.slice_in_dim(x, 0, extent - amount, axis=axis)], axis=axis)


class Scatter:
    def __init__(self, me, part, acc, bufs, sems, piece):
        self.me, self.part, self.acc, self.piece = me, part, acc, piece
        self.r0, self.r = bufs[0], bufs[1:]
        self.csend, self.crecv, self.send, self.recv = sems

    def core_copy(self, mask):
        block = flip_mask(flip(self.me, 1), mask)
        return remote(self.part(block), self.r0.at[mask], self.csend.at[mask], self.crecv.at[mask], flip(self.me, 1))

    def phase_copy(self, c, phase, rel):
        order = colour_order(c)
        absmask = sum(1 << order[pos] for pos in range(3) if (rel >> pos) & 1)
        low = rel >> (phase + 1)
        sem = (0, 4, 6)[phase] + low
        return remote(self.piece(self.acc.at[absmask], c), self.piece(self.r[phase].at[low], c),
                      self.send.at[c, sem], self.recv.at[c, sem], flip(self.me, STRIDES[order[phase]]))

    def core_start(self):
        for mask in range(7, -1, -1):
            self.core_copy(mask).start()

    def core_done(self, mask):
        self.core_copy(mask).wait_recv()
        self.acc[mask] = self.part(flip_mask(self.me, mask))[...] + self.r0[mask]
        for c in range(3):
            if (mask >> c) & 1:
                order = colour_order(c)
                rel = sum(1 << pos for pos in range(3) if (mask >> order[pos]) & 1)
                self.phase_copy(c, 0, rel).start()

    def phase_done(self, c, phase, low):
        order = colour_order(c)
        rel = low << (phase + 1)
        self.phase_copy(c, phase, rel | (1 << phase)).wait_recv()
        absmask = sum(1 << order[pos] for pos in range(3) if (rel >> pos) & 1)
        dst = self.piece(self.acc.at[absmask], c)
        dst[...] = dst[...] + self.piece(self.r[phase].at[low], c)[...]

    def move_on(self, c, phase, rel):
        self.phase_copy(c, phase, rel).start()

    def steps(self):
        out = [functools.partial(self.core_done, mask) for mask in range(7, -1, -1)]

        def phase0(c, low):
            self.phase_done(c, 0, low)
            if low & 1:
                self.move_on(c, 1, low << 1)

        def phase1(c, low):
            self.phase_done(c, 1, low)
            if low & 1:
                self.move_on(c, 2, low << 2)

        for low in (3, 1, 2, 0):
            out += [functools.partial(phase0, c, low) for c in range(3)]
        for low in (1, 0):
            out += [functools.partial(phase1, c, low) for c in range(3)]
        out += [functools.partial(self.phase_done, c, 2, 0) for c in range(3)]
        return out

    def finish(self):
        for mask in range(8):
            self.core_copy(mask).wait_send()
        for c in range(3):
            for phase in range(3):
                for low in range(4 >> phase):
                    self.phase_copy(c, phase, (low << (phase + 1)) | (1 << phase)).wait_send()


ROW_PIECES = ((0, 96), (96, 80), (176, 80))


def row_piece(ref, c):
    start, size = ROW_PIECES[c]
    return ref.at[pl.ds(start, size)]


def col_piece(ref, c):
    return ref.at[:, pl.ds(c * (DF // 3), DF // 3)]


def step_kernel(tok, gain, wq, wk, wv, dq, dk, dv, table, tok_o, w_o, g, qkv_o, dx_o, dw_o, dg_o,
                wpad, d, ids, tok_v, tok_row, gain_p, gain_v, gain8, rows, xp, xacc, x0, x1, x2, x3, w0, w1, w2, w3, dgp, dgsum, dgall,
                tabsem, loc, gsem, dxsem, small_send, small_recv, dgs, dgr, gws, gwr, gwcs, gwcr, gds, gdr, gdcs, gdcr,
                xcs, xcr, xs, xr, wcs, wcr, ws, wr):
    me = lax.axis_index(AXIS_NAME)
    vocab = table.shape[0]
    tiles = DM // 128
    for ref, src in ((wpad, (wq, wk, wv)), (d, (dq, dk, dv))):
        height = src[0].shape[0]
        ref[:height, :DM] = src[0][...].astype(BF16)
        ref[:height, DM:DM + 128] = src[1][...].astype(BF16)
        ref[:height, DM + 128:] = src[2][...].astype(BF16)
    w = wpad.at[pl.ds(0, WROWS)]
    gain_p[...] = jnp.zeros_like(gain_p)
    gain_p[0:1, 0:WROWS] = gain[...]
    gain_v[...] = jnp.zeros_like(gain_v)
    gain_v[me] = gain_p[...]
    dgall[...] = jnp.zeros_like(dgall)
    dgp[...] = jnp.zeros_like(dgp)
    tok_v[me] = tok[...]
    wg = Gather(me, w, WRows(w_o), (gws, gwr, gwcs, gwcr), DF // 3)
    dg = Gather(me, d, g, (gds, gdr, gdcs, gdcr), DF // 3)
    xrs = Scatter(me, lambda b: xp.at[b], xacc, (x0, x1, x2, x3), (xcs, xcr, xs, xr), row_piece)
    own = [pltpu.make_async_copy(w, w_o.at[pl.ds(pl.multiple_of(me * WROWS, 8), WROWS)], loc.at[0]),
           pltpu.make_async_copy(d, g.at[me], loc.at[1])]
    tok_copies, gain_copies = [], []
    for k in range(1, NDEV):
        dev = (me + k) % NDEV
        tok_copies.append(remote(tok, tok_v.at[me], small_send.at[0, k], small_recv.at[0, k], dev))
        gain_copies.append(remote(gain_p.at[pl.ds(0, 1)], gain_v.at[me, pl.ds(0, 1)], small_send.at[1, k], small_recv.at[1, k], dev))

    def piece(gather, c, mask):
        gather.wait_piece(c, mask)
        gather.start_piece(c, mask)

    def pieces(mask):
        return [functools.partial(piece, gather, c, mask) for gather in (wg, dg) for c in range(3)]

    def gather_rows(tab):
        table_copies = [pltpu.make_async_copy(table.at[:, pl.ds(s * 128, 128)], tab.at[pl.ds(0, vocab), s], tabsem.at[s])
                        for s in range(tiles)]
        for copy in table_copies:
            copy.start()
        tab[vocab] = jnp.zeros((8, 128), F32)
        barrier_all(me)
        for copy in tok_copies + gain_copies:
            copy.start()
        for gather in (wg, dg):
            for c in range(3):
                gather.start_piece(c, 0)
        for copy in own:
            copy.start()
        for copy in tok_copies:
            copy.wait()
        local = tok_v[...] - me * vocab
        tok_row[...] = jnp.where((local >= 0) & (local < vocab), local, vocab)
        ids_copy = pltpu.make_async_copy(tok_row, ids, loc.at[2])
        ids_copy.start()
        tok_o[...] = tok_v[...]
        for copy in gain_copies:
            copy.wait()
        total = jnp.zeros((8, DM), F32)
        for k in range(NDEV):
            wide = jnp.concatenate([gain_v[k], jnp.zeros((8, DM - 128), F32)], axis=1)
            total = total + (rotate(wide, k * WROWS, 1) if k else wide)
        gain8[...] = total
        ids_copy.wait()
        for copy in table_copies:
            copy.wait()
        for event in pieces(1):
            event()
        when = {2: pieces(2), 7: pieces(3)[:3], 9: pieces(3)[3:]}

        @pl.loop(0, NDEV)
        def _(k):
            base = me + (1 - k // 8) * (1 - 2 * (me % 2))
            mask = 7 - k % 8
            b = base
            for bit, stride in enumerate(STRIDES):
                b = b + stride * (1 - 2 * ((base // stride) % 2)) * ((mask // (1 << bit)) % 2)

            @pl.loop(0, SEQ // 16)
            def _(i):
                for j in range(16):
                    rows[i * 16 + j] = tab[ids[b, 0, i * 16 + j]]

            for s in range(tiles):
                xp[b, :, s * 128:(s + 1) * 128] = rows[:, s, :].astype(BF16)
            for at in range(NDEV):
                group = when.get(at, [])
                if at >= 1 and at <= 8:
                    group = [lambda at=at: xrs.core_copy(8 - at).start()] + group
                if group:
                    @pl.when(k == at)
                    def _(group=group):
                        for event in group:
                            event()

    pl.run_scoped(gather_rows, pltpu.VMEM((vocab + 1, 8, 128), F32))
    events = xrs.steps()
    for event in events[:8]:
        event()
    for mask in range(4, 8):
        for event in pieces(mask):
            event()
    wg.finish()
    dg.finish()
    for copy in own:
        copy.wait()
    events = events[8:]

    def finish_step(wfull, gbuf, dxbuf, dwp, wacc):
        load = lambda t, slot: pltpu.make_async_copy(g.at[pl.ds(PAIR * t, PAIR)], gbuf.at[slot], gsem.at[slot])
        store = lambda t, slot: pltpu.make_async_copy(dxbuf.at[slot], dx_o.at[pl.ds(STEP * t, STEP)], dxsem.at[slot])
        w_copy = pltpu.make_async_copy(w_o, wfull, loc.at[3])
        w_copy.start()
        load(0, 0).start()
        part = lambda b: dwp.at[pl.ds(pl.multiple_of(b * WROWS, 8), WROWS)]
        wrs = Scatter(me, part, wacc, (w0, w1, w2, w3), (wcs, wcr, ws, wr), col_piece)

        def weight_grads():
            x = xacc[0].astype(F32)
            r = lax.rsqrt(jnp.mean(x * x, axis=-1, keepdims=True) + 1e-5)
            n = (x * r * gain8[...][0:1]).astype(BF16)
            dwp[...] = lax.dot_general(n, d[...], (((0,), (0,)), ((), ())), preferred_element_type=F32)
            wrs.core_start()
            qkv_o[...] = jnp.dot(n, wfull[...], preferred_element_type=F32).astype(BF16)

        slots = NDEV // PAIR * QUARTERS
        groups = [events[len(events) * k // SPLIT:len(events) * (k + 1) // SPLIT] for k in range(SPLIT)] + [[weight_grads]]
        later = wrs.steps()
        rest = slots - SPLIT - 1
        groups += [later[len(later) * k // rest:len(later) * (k + 1) // rest] for k in range(rest)]
        w_copy.wait()

        @pl.loop(0, NDEV // PAIR)
        def _(t):
            slot = t % 2

            @pl.when(t + 1 < NDEV // PAIR)
            def _():
                load(t + 1, 1 - slot).start()

            load(t, slot).wait()

            @pl.when(t >= 2)
            def _():
                store(t - 2, slot).wait()

            dxbuf[slot] = lax.dot_general(gbuf[slot].reshape(STEP, DF), wfull[...], (((1,), (1,)), ((), ())),
                                          preferred_element_type=F32)

            def chunk(q):
                at = pl.ds(pl.multiple_of(q * CHUNK, CHUNK), CHUNK)
                dn = dxbuf[slot, at]
                per = SEQ // CHUNK
                x = xp[PAIR * t + q // per, pl.ds(pl.multiple_of((q % per) * CHUNK, CHUNK), CHUNK)].astype(F32)
                r = lax.rsqrt(jnp.mean(x * x, axis=-1, keepdims=True) + 1e-5)
                h = x * r
                dgp[...] += jnp.sum((dn * h).reshape(CHUNK // 8, 8, DM), axis=0)
                u = dn * gain8[...][0:1]
                dxbuf[slot, at] = r * (u - h * jnp.mean(u * h, axis=-1, keepdims=True))

            for part_of in range(QUARTERS):
                pl.loop(part_of * (STEP // CHUNK) // QUARTERS, (part_of + 1) * (STEP // CHUNK) // QUARTERS)(chunk)
                for step in range(NDEV // PAIR):
                    group = groups[step * QUARTERS + part_of]
                    if group:
                        @pl.when(t == step)
                        def _(group=group):
                            for event in group:
                                event()

            store(t, slot).start()

        dgsum[...] = jnp.broadcast_to(jnp.sum(dgp[...], axis=0, keepdims=True), dgsum.shape)
        dgall[me] = dgsum[...]
        small = [remote(dgsum.at[pl.ds(0, 1)], dgall.at[me, pl.ds(0, 1)], dgs.at[k], dgr.at[k], (me + k) % NDEV)
                 for k in range(1, NDEV)]
        for copy in small:
            copy.start()
        dw_o[...] = wacc[0]
        for copy in small:
            copy.wait()
        dg_o[...] = jnp.sum(dgall[...], axis=0)
        store(NDEV // PAIR - 2, 0).wait()
        store(NDEV // PAIR - 1, 1).wait()
        wrs.finish()

    vmem = pltpu.VMEM
    pl.run_scoped(finish_step, vmem((DM, DF), BF16), vmem((2, PAIR, SEQ, DF), BF16), vmem((2, STEP, DM), F32),
                  vmem((DM, DF), F32), vmem((8, WROWS, DF), F32))
    xrs.finish()


class WRows:
    def __init__(self, ref):
        self.ref = ref

    @property
    def at(self):
        return self

    def __getitem__(self, index):
        device, _, cols = index
        return self.ref.at[pl.ds(pl.multiple_of(device * WROWS, 8), WROWS), cols]


def step_all(tok, gain, weights, grads, table):
    vm = pl.BlockSpec(memory_space=pltpu.VMEM)
    hbm = pl.BlockSpec(memory_space=pl.ANY)
    dma = pltpu.SemaphoreType.DMA
    vmem = pltpu.VMEM
    sds = jax.ShapeDtypeStruct
    xb = lambda k: vmem((k, SEQ, DM), BF16)
    wb = lambda k: vmem((k, WROWS, DF), F32)
    return pl.pallas_call(
        step_kernel,
        out_shape=(sds((NDEV, 1, SEQ), jnp.int32), sds((DM, DF), BF16), sds((NDEV, SEQ, DF), BF16), sds((SEQ, DF), BF16),
                   sds((NDEV * SEQ, DM), F32), sds((WROWS, DF), F32), sds((8, DM), F32)),
        in_specs=[vm] * 8 + [hbm],
        out_specs=(vm, hbm, hbm, vm, hbm, vm, vm),
        scratch_shapes=[vmem((64, DF), BF16), vmem((SEQ, DF), BF16), pltpu.SMEM((NDEV, 1, SEQ), jnp.int32),
                        vmem((NDEV, 1, SEQ), jnp.int32), vmem((NDEV, 1, SEQ), jnp.int32), vmem((8, 128), F32), vmem((NDEV, 8, 128), F32), vmem((8, DM), F32),
                        vmem((SEQ, 8, 128), F32), xb(NDEV), xb(8), xb(8), xb(4), xb(2), xb(1), wb(8), wb(4), wb(2), wb(1),
                        vmem((8, DM), F32), vmem((8, DM), F32), vmem((NDEV, 8, DM), F32),
                        dma((8,)), dma((4,)), dma((2,)), dma((2,)), dma((2, NDEV)), dma((2, NDEV)), dma((NDEV,)), dma((NDEV,))]
        + [dma((3, 8))] * 8 + [dma((8,)), dma((8,)), dma((3, 7)), dma((3, 7))] * 2,
        compiler_params=pltpu.CompilerParams(collective_id=0, has_side_effects=True, vmem_limit_bytes=67043328),
        name="step_all",
    )(tok, gain, *weights, *grads, table)


def embed_kernel(keys, starts, dx, qkv, dw, dg, de_o, q_o, k_o, v_o, dwq_o, dwk_o, dwv_o, dg_o, dxv, de, insem, outsem):
    vocab = de_o.shape[0]
    fetch = pltpu.make_async_copy(dx, dxv.at[pl.ds(0, NDEV * SEQ)], insem)
    fetch.start()

    @pl.loop(0, (vocab + 8) // 32)
    def _(i):
        de[pl.ds(pl.multiple_of(i * 32, 32), 32)] = jnp.zeros((32, DM), F32)

    for outs, ref in (((q_o, k_o, v_o), qkv), ((dwq_o, dwk_o, dwv_o), dw)):
        outs[0][...] = ref[:, :DM]
        outs[1][...] = ref[:, DM:DM + 128]
        outs[2][...] = ref[:, DM + 128:]
    dg_o[...] = dg[...][0:1]
    fetch.wait()
    top = starts[0, 0] - 1

    def token(p, carry):
        prev, total = carry
        key = keys[p]
        row = lax.shift_right_logical(key, 12)
        total = jnp.where(row == prev, total, 0.0) + dxv[pl.ds(key & 4095, 1), :]
        de[pl.ds(row, 1), :] = total
        return row, total

    def group(i, carry):
        first = (top - i) * 8
        for j in range(7, -1, -1):
            carry = token(first + j, carry)
        return carry

    def two_groups(i, carry):
        return group(2 * i + 1, group(2 * i, carry))

    carry = (jnp.int32(-1), jnp.zeros((1, DM), F32))
    done = jnp.int32(0)
    copies = []
    bounds = embed_bounds(vocab)
    for k in range(len(bounds) - 1):
        low, high = bounds[k + 1], bounds[k]
        upto = top + 1 - starts[0, k + 1]
        even = lax.shift_right_logical(done + 1, 1)
        carry = lax.fori_loop(done, jnp.minimum(even * 2, upto), group, carry)
        last = jnp.maximum(lax.shift_right_logical(upto, 1), even)
        carry = lax.fori_loop(even, last, two_groups, carry)
        carry = lax.fori_loop(jnp.maximum(last * 2, done), upto, group, carry)
        done = upto
        copies.append(pltpu.make_async_copy(de.at[pl.ds(low, high - low)], de_o.at[pl.ds(low, high - low)], outsem.at[k]))
        copies[-1].start()
    for copy in copies:
        copy.wait()


def embed_bounds(vocab):
    blocks = 16
    return [vocab] + [(vocab * k // blocks) // 8 * 8 for k in range(blocks - 1, 0, -1)] + [0]


def embed_all(local, dx, qkv, dw, dg, vocab):
    order = jnp.arange(NDEV * SEQ, dtype=jnp.int32)
    keys = jnp.sort(jnp.where((local >= 0) & (local < vocab), local, vocab).reshape(-1) * 4096 + order)
    bounds = jnp.array(embed_bounds(vocab), jnp.int32)
    below = jnp.sum((keys[None, :] < bounds[:, None] * 4096).astype(jnp.int32), axis=1)
    starts = jnp.concatenate([(below[:1] + 7) // 8, below[1:] // 8])[None]
    vm = pl.BlockSpec(memory_space=pltpu.VMEM)
    hbm = pl.BlockSpec(memory_space=pl.ANY)
    smem = pl.BlockSpec(memory_space=pltpu.SMEM)
    sds = jax.ShapeDtypeStruct
    dma = pltpu.SemaphoreType.DMA
    return pl.pallas_call(
        embed_kernel,
        out_shape=(sds((vocab, DM), F32), sds((SEQ, DM), BF16), sds((SEQ, 128), BF16), sds((SEQ, 128), BF16),
                   sds((WROWS, DM), F32), sds((WROWS, 128), F32), sds((WROWS, 128), F32), sds((1, WROWS), F32)),
        in_specs=[smem, smem, hbm, vm, vm, vm],
        out_specs=(hbm,) + (vm,) * 7,
        scratch_shapes=[pltpu.VMEM((NDEV * SEQ + 8, DM), F32), pltpu.VMEM((vocab + 8, DM), F32), dma, dma((16,))],
        compiler_params=pltpu.CompilerParams(vmem_limit_bytes=62 * 2**20),
        name="embed_all",
    )(keys, starts, dx, qkv, dw, dg)


def solution(mesh):
    def local_step(tokens, embed_shard, gain_shard, wq_shard, wk_shard, wv_shard, d_query, d_key, d_value):
        vocab_local = embed_shard.shape[0]
        tok_all, _, _, qkv, dx_all, dw, dgain = step_all(
            tokens, gain_shard[None], (wq_shard, wk_shard, wv_shard), (d_query[0], d_key[0], d_value[0]), embed_shard)
        dgain = lax.dynamic_slice(dgain, (0, lax.axis_index(AXIS_NAME) * WROWS), (8, WROWS))
        d_embed, *small = embed_all(tok_all - lax.axis_index(AXIS_NAME) * vocab_local, dx_all, qkv, dw, dgain, vocab_local)
        return (*(a[None] for a in small[:3]), d_embed, small[6][0], *small[3:6])

    row_spec = P(AXIS_NAME, None)
    act_spec = P(AXIS_NAME, None, None)
    vec_spec = P(AXIS_NAME)
    return jax.shard_map(local_step, mesh=mesh,
                         in_specs=(row_spec, row_spec, vec_spec, row_spec, row_spec, row_spec, act_spec, act_spec, act_spec),
                         out_specs=(act_spec, act_spec, act_spec, row_spec, vec_spec, row_spec, row_spec, row_spec),
                         check_vma=False)
```
